8 devices in a mesh: rep: 2 (over y, z), dp: 4 (over x, core).
Axes of the slice: x: 2, y: 2, z: 1, core: 2. Of those that a mesh axis runs over, the one named last changes fastest.
Arguments:
- g_w_gate: bfloat16 [8, 2, 1024, 3584], P(('rep', 'dp')), parts along dimension 0
- g_w_up: bfloat16 [8, 2, 1024, 3584], P(('rep', 'dp')), parts along dimension 0
- g_w_down: bfloat16 [8, 2, 3584, 1024], P(('rep', 'dp')), parts along dimension 0
- w_gate: bfloat16 [2, 1024, 3584], replicated
- w_up: bfloat16 [2, 1024, 3584], replicated
- w_down: bfloat16 [2, 3584, 1024], replicated
- m_w_gate: float32 [2, 1024, 3584], P(None, 'dp')
- m_w_up: float32 [2, 1024, 3584], P(None, 'dp')
- m_w_down: float32 [2, 3584, 1024], P(None, 'dp')
- v_w_gate: float32 [2, 1024, 3584], P(None, 'dp')
- v_w_up: float32 [2, 1024, 3584], P(None, 'dp')
- v_w_down: float32 [2, 3584, 1024], P(None, 'dp')
Outputs:
- output 1: bfloat16 [4, 1024, 3584], P('rep'), parts along dimension 0
- output 2: bfloat16 [4, 1024, 3584], P('rep'), parts along dimension 0
- output 3: bfloat16 [4, 3584, 1024], P('rep'), parts along dimension 0
- output 4: float32 [4, 1024, 3584], P('rep', 'dp'), parts along dimension 0
- output 5: float32 [4, 1024, 3584], P('rep', 'dp'), parts along dimension 0
- output 6: float32 [4, 3584, 1024], P('rep', 'dp'), parts along dimension 0
- output 7: float32 [4, 1024, 3584], P('rep', 'dp'), parts along dimension 0
- output 8: float32 [4, 1024, 3584], P('rep', 'dp'), parts along dimension 0
- output 9: float32 [4, 3584, 1024], P('rep', 'dp'), parts along dimension 0
There are 2 independent parts. The reference program is written for one: setup_inputs(seed, part) draws one part's arguments, and reference() takes and returns one part's arrays. A program takes and returns all parts, laid end to end along the dimension named above; an argument that names none is the same for every part.
All inputs are finite; a program needn't handle non-finite values.
Results may differ from the reference program's by a relative error of at most 0.022.
Values are sent between devices in bfloat16 or wider.
A program may use at most 2 GiB of HBM per device.

```python
import jax
import jax.numpy as jnp
from jax import lax

DEVICES = 4
D = 1024
FF = 3584
LAYERS = 2
NAMES = ("w_gate", "w_up", "w_down")
SHAPES = {"w_gate": (LAYERS, D, FF), "w_up": (LAYERS, D, FF), "w_down": (LAYERS, FF, D)}


def setup_inputs(seed: int = 0, part: int = 0) -> dict:
    kz, *keys = jax.random.split(jax.random.key(seed), 1 + 5 * len(NAMES))
    loud = 2.0 ** jax.random.uniform(kz, (), jnp.float32, -1.0, 1.0)
    drawn = {}
    for name, key, both in zip(NAMES, keys[:3], keys[3:6], strict=True):
        own = jax.random.normal(jax.random.fold_in(key, part), (DEVICES, *SHAPES[name]), jnp.float32)
        shared = jax.random.normal(jax.random.fold_in(both, part), SHAPES[name], jnp.float32)
        drawn["g_" + name] = (loud * (0.7 * shared / DEVICES + 0.7 * own * DEVICES**-0.5)).astype(jnp.bfloat16)
    for name, key in zip(NAMES, keys[6:9], strict=True):
        drawn[name] = (jax.random.normal(key, SHAPES[name], jnp.float32) * SHAPES[name][1] ** -0.5).astype(jnp.bfloat16)
    for name, key in zip(NAMES, keys[9:12], strict=True):
        drawn["m_" + name] = loud * 0.5 * jax.random.normal(key, SHAPES[name], jnp.float32)
    for name, key in zip(NAMES, keys[12:15], strict=True):
        drawn["v_" + name] = loud * loud * jax.random.uniform(key, SHAPES[name], jnp.float32, 0.5, 1.5)
    return drawn


def adamw(w, m, v, g):
    m = 0.9 * m + 0.1 * g
    v = 0.95 * v + 0.05 * g * g
    step = m * lax.rsqrt(v + 1e-8) + 0.1 * w
    return (w - 0.02 * step).astype(jnp.bfloat16), m, v


def reference(g_w_gate, g_w_up, g_w_down, w_gate, w_up, w_down, m_w_gate, m_w_up, m_w_down, v_w_gate, v_w_up, v_w_down):
    def total(terms):
        return lax.scan(lambda so_far, term: (so_far + term.astype(jnp.float32), None), jnp.zeros(terms.shape[1:], jnp.float32), terms)[0]

    gradients = [total(terms).astype(jnp.bfloat16).astype(jnp.float32) for terms in (g_w_gate, g_w_up, g_w_down)]
    new = [
        adamw(w.astype(jnp.float32), m, v, g)
        for w, m, v, g in zip((w_gate, w_up, w_down), (m_w_gate, m_w_up, m_w_down), (v_w_gate, v_w_up, v_w_down), gradients, strict=True)
    ]
    return tuple(one[which] for which in range(3) for one in new)
```

```python
import jax
import jax.numpy as jnp
from jax import lax
from jax.experimental import pallas as pl
from jax.experimental.pallas import tpu as pltpu
from jax.sharding import PartitionSpec as P


CORES = [(0, 1), (1, 0), (2, 3), (3, 2)]
CHIPS = [(0, 2), (2, 0), (1, 3), (3, 1)]

REDUCED = (
    ((0, 0, 64), (0, 64, 192), (1, 0, 256)),
    ((0, 0, 256), (1, 0, 256)),
    ((0, 0, 896), (1, 0, 896)),
)
GATHERED = (
    ((0, 0, 256), (1, 0, 256)),
    ((0, 0, 256), (1, 0, 256)),
    ((0, 0, 896), (1, 0, 512), (1, 512, 256), (1, 768, 128)),
)


def partners():
    me = lax.axis_index("dp")
    return me, me + 1 - 2 * (me % 2), (me + 2) % 4, 3 - me


def adamw(w, m, v, g):
    m = 0.9 * m + 0.1 * g
    v = 0.95 * v + 0.05 * g * g
    step = m * lax.rsqrt(v + 1e-8) + 0.1 * w
    return (w - 0.02 * step).astype(jnp.bfloat16), m, v


def place(shape, block, items, out=None):
    arrays = [one[0] for one in items]
    n = len(items)

    def kernel(*refs):
        pieces, refs = refs[:n], refs[n + (out is not None) :]
        whole, buffers, (read, wrote) = refs[0], refs[1 : 1 + n], refs[1 + n :]
        owners = partners()
        takes = [pltpu.make_async_copy(pieces[i], buffers[i], read.at[i]) for i in range(n)]
        for take in takes:
            take.start()
        puts = []
        for i, (array, who, layer, first) in enumerate(items):
            rows = pl.ds(pl.multiple_of(owners[who] * block + first, 16), array.shape[-2])
            put = pltpu.make_async_copy(buffers[i], whole.at[layer, rows], wrote.at[i])
            takes[i].wait()
            put.start()
            puts.append(put)
        for put in puts:
            put.wait()

    size = sum(a.size for a in arrays)
    anywhere = pl.BlockSpec(memory_space=pl.ANY)
    more = () if out is None else (out,)
    return pl.pallas_call(
        kernel,
        out_shape=jax.ShapeDtypeStruct(shape, jnp.bfloat16),
        in_specs=[anywhere] * (n + len(more)),
        out_specs=anywhere,
        scratch_shapes=[pltpu.VMEM(a.shape, a.dtype) for a in arrays] + [pltpu.SemaphoreType.DMA((n,))] * 2,
        input_output_aliases={n: 0} if more else {},
        cost_estimate=pl.CostEstimate(flops=size * 8, bytes_accessed=4 * size, transcendentals=0),
        name="place",
    )(*arrays, *more)


def solution(mesh):
    def step(*arrays):
        terms, weights, ms, vs = (arrays[i : i + 3] for i in (0, 3, 6, 9))
        me, core, chip, both = partners()

        def part(array, who, piece, block):
            layer, first, rows = piece
            at = (0,) * (array.ndim - 3) + (layer, who * block + first, 0)
            sizes = (1,) * (array.ndim - 2) + (rows, array.shape[-1])
            return lax.dynamic_slice(array, at, sizes).reshape(rows, array.shape[-1])

        f32 = jnp.float32
        near, far = [], []
        for term, m, pieces in zip(terms, ms, REDUCED, strict=True):
            block = m.shape[1]
            for piece in pieces:
                theirs = lax.ppermute(part(term, both, piece, block), "dp", CORES)
                total = (part(term, chip, piece, block).astype(f32) + theirs.astype(f32)).astype(jnp.bfloat16)
                far.append(lax.ppermute(total, "dp", CHIPS))
            own = lax.dynamic_slice_in_dim(term[0], core * block, block, 1)
            near.append(lax.ppermute(own, "dp", CORES))

        new = []
        for i, (term, w, m, v, pieces) in enumerate(zip(terms, weights, ms, vs, REDUCED, strict=True)):
            block = m.shape[1]
            arrived = [far.pop(0) for _ in pieces]
            other = jnp.concatenate(arrived, 0).reshape(m.shape)
            own = lax.dynamic_slice_in_dim(term[0], me * block, block, 1)
            g = lax.reduce_precision(own.astype(f32) + near[i].astype(f32) + other.astype(f32), 8, 7)
            mine = lax.dynamic_slice_in_dim(w, me * block, block, 1).astype(f32)
            new.append(adamw(mine, m, v, g))

        wholes = []
        for i, ((w, _, _), weight, pieces) in enumerate(zip(new, weights, GATHERED, strict=True)):
            block = w.shape[1]
            beside = lax.ppermute(w, "dp", CORES)
            items = [(x[layer], who, layer, 0) for x, who in ((w, 0), (beside, 1)) for layer in (0, 1)]
            out = place(weight.shape, block, items)
            late = []
            for layer, first, rows in pieces:
                across = lax.ppermute(w[layer, first : first + rows], "dp", CHIPS)
                late.append(((across, 2, layer, first), (lax.ppermute(across, "dp", CORES), 3, layer, first)))
            if i < 2:
                out = place(weight.shape, block, [item for pair in late for item in pair], out)
            else:
                for pair in late:
                    out = place(weight.shape, block, list(pair), out)
            wholes.append(out)
        return (*wholes, *(one[1] for one in new), *(one[2] for one in new))

    all_of, cut = P(None, None, None), P(None, "dp", None)
    return jax.shard_map(
        step,
        mesh=mesh,
        in_specs=(P(("rep", "dp"), None, None, None),) * 3 + (all_of,) * 3 + (cut,) * 6,
        out_specs=(P("rep", None, None),) * 3 + (P("rep", "dp", None),) * 6,
        check_vma=False,
    )
```

```python
import jax
import jax.numpy as jnp
from jax import lax
from jax.experimental import pallas as pl
from jax.experimental.pallas import tpu as pltpu
from jax.sharding import PartitionSpec as P


CORES = [(0, 1), (1, 0), (2, 3), (3, 2)]
CHIPS = [(0, 2), (2, 0), (1, 3), (3, 1)]

FIRST = ((0, 0, 64), (0, 64, 192), (1, 0, 256))
LAST = ((0, 0, 896), (1, 0, 512), (1, 512, 256), (1, 768, 128))


def partners():
    me = lax.axis_index("dp")
    return me, me + 1 - 2 * (me % 2), (me + 2) % 4, 3 - me


def adamw(w, m, v, g):
    m = 0.9 * m + 0.1 * g
    v = 0.95 * v + 0.05 * g * g
    step = m * lax.rsqrt(v + 1e-8) + 0.1 * w
    return (w - 0.02 * step).astype(jnp.bfloat16), m, v


def place(shape, block, items, out=None):
    arrays = [one[0] for one in items]
    n = len(items)
    more = () if out is None else (out,)

    def kernel(*refs):
        pieces, refs = refs[:n], refs[n + len(more) :]
        whole, buffers, (read, wrote) = refs[0], refs[1 : 1 + n], refs[1 + n :]
        owners = partners()
        takes = [pltpu.make_async_copy(pieces[i], buffers[i], read.at[i]) for i in range(n)]
        for take in takes:
            take.start()
        puts = []
        for i, (array, who, layer, first) in enumerate(items):
            rows = pl.ds(pl.multiple_of(owners[who] * block + first, 16), array.shape[-2])
            put = pltpu.make_async_copy(buffers[i], whole.at[layer, rows] if array.ndim == 2 else whole.at[:, rows], wrote.at[i])
            takes[i].wait()
            put.start()
            puts.append(put)
        for put in puts:
            put.wait()

    size = sum(a.size for a in arrays)
    anywhere = pl.BlockSpec(memory_space=pltpu.HBM)
    return pl.pallas_call(
        kernel,
        out_shape=jax.ShapeDtypeStruct(shape, jnp.bfloat16),
        in_specs=[anywhere] * (n + len(more)),
        out_specs=anywhere,
        scratch_shapes=[pltpu.VMEM(a.shape, a.dtype) for a in arrays] + [pltpu.SemaphoreType.DMA((n,))] * 2,
        input_output_aliases={} if out is None else {n: 0},
        cost_estimate=pl.CostEstimate(flops=size * 8, bytes_accessed=4 * size, transcendentals=0),
        name="place",
    )(*arrays, *more)


def solution(mesh):
    def step(*arrays):
        terms, weights, ms, vs = (arrays[i : i + 3] for i in (0, 3, 6, 9))
        me, core, chip, both = partners()
        f32 = jnp.float32

        def part(array, who, piece, block):
            if piece is None:
                return lax.dynamic_slice_in_dim(array[0], who * block, block, 1)
            layer, first, rows = piece
            at = (0, layer, who * block + first, 0)
            return lax.dynamic_slice(array, at, (1, 1, rows, array.shape[-1])).reshape(rows, array.shape[-1])

        def send(array, pairs):
            return lax.ppermute(array, "dp", pairs)

        gate, up, down = terms
        far = []
        for n, piece in (*((0, piece) for piece in FIRST), (1, None), (2, None)):
            block = ms[n].shape[1]
            mine = part(terms[n], both, piece, block)
            theirs = send(mine, CORES)
            total = (part(terms[n], chip, piece, block).astype(f32) + theirs.astype(f32)).astype(jnp.bfloat16)
            far.append(send(total, CHIPS))
        far = [jnp.concatenate(far[:3], 0).reshape(ms[0].shape), *far[3:]]
        near = []
        for term, m in zip(terms, ms, strict=True):
            theirs = part(lax.optimization_barrier((term, total))[0], core, None, m.shape[1])
            near.append(send(theirs, CORES))

        new, wholes = [], []
        for term, w, m, v, other, beside, n in zip(terms, weights, ms, vs, far, near, range(3), strict=True):
            block = m.shape[1]
            own = part(term, me, None, block)
            g = lax.reduce_precision(own.astype(f32) + beside.astype(f32) + other.astype(f32), 8, 7)
            new.append(adamw(lax.dynamic_slice_in_dim(w, me * block, block, 1).astype(f32), m, v, g))
            out = new[-1][0]
            across = [send(out, CHIPS)] if n < 2 else []
            beside = send(out, CORES)
            whole = place(w.shape, block, [(out, 0, slice(None), 0), (beside, 1, slice(None), 0)])
            if n < 2:
                items = [(across[0], 2, slice(None), 0), (send(across[0], CORES), 3, slice(None), 0)]
                whole = place(w.shape, block, items, whole)
            else:
                for layer, row, rows in LAST:
                    across = send(out[layer, row : row + rows], CHIPS)
                    items = [(across, 2, layer, row), (send(across, CORES), 3, layer, row)]
                    whole = place(w.shape, block, items, whole)
            wholes.append(whole)
        return (*wholes, *(one[1] for one in new), *(one[2] for one in new))

    all_of, cut = P(None, None, None), P(None, "dp", None)
    return jax.shard_map(
        step,
        mesh=mesh,
        in_specs=(P(("rep", "dp"), None, None, None),) * 3 + (all_of,) * 3 + (cut,) * 6,
        out_specs=(P("rep", None, None),) * 3 + (P("rep", "dp", None),) * 6,
        check_vma=False,
    )
```
